32 devices in a mesh: member: 2 (over x), node: 16 (over z, y, core).
Axes of the slice: x: 2, y: 2, z: 4, core: 2. Of those that a mesh axis runs over, the one named last changes fastest.
Arguments:
- conditioning: bfloat16 [168, 32768], P(None, ('member', 'node')), parts along dimension 1, may hold values from -6 to 6
- target_state: float32 [84, 32768], P(None, ('member', 'node')), parts along dimension 1, may hold values from -6 to 6
- noise_sample: float32 [84, 32768], P(None, ('member', 'node')), parts along dimension 1, may hold values from -6 to 6
- step_index: int32 [2], P('member'), parts along dimension 0, may hold values from 0 to 19
- mesh_features: float32 [3, 10240], P(None, 'node'), may hold values from -1 to 1
- edge_geometry: float32 [4, 65536], P(None, 'node'), may hold values from -6 to 6
- edge_slot: int32 [65536], P('node'), may hold values from 0 to 255, as said below
- edge_receiver: int32 [65536], P('node'), may hold values from 0 to 639
- send_rows: int32 [256, 16], P('node'), may hold values from 0 to 1023
- edge_count: int32 [16], P('node'), may hold values from 1399 to 4096, as said below
- embed_weight: bfloat16 [252, 512], replicated, may hold values from -0.375 to 0.375
- mesh_weight: float32 [3, 512], replicated, may hold values from -3.5 to 3.5
- geom_weight: float32 [4, 512], replicated, may hold values from -3 to 3
- sender_weight: bfloat16 [512, 512], P('node'), may hold values from -0.15625 to 0.15625
- edge_weight: bfloat16 [512, 512], P('node'), may hold values from -0.15625 to 0.15625
- receiver_weight: bfloat16 [512, 512], P('node'), may hold values from -0.15625 to 0.15625
- message_weight: bfloat16 [512, 512], P('node'), may hold values from -0.25 to 0.25
- node_weight: bfloat16 [1024, 512], P('node'), may hold values from -0.1875 to 0.1875
- output_weight: bfloat16 [512, 512], P('node'), may hold values from -0.25 to 0.25
- noise_weight: float32 [32, 512], replicated, may hold values from -1 to 1
- film_weight: bfloat16 [512, 2048], replicated, may hold values from -0.25 to 0.25
Outputs:
- mesh_latent: bfloat16 [10240, 1024], P('node', 'member'), parts along dimension 1
The draws below stay inside these ranges and needn't reach their ends.
There are 2 independent parts, one for each index of `member`. The reference program is written for one: setup_inputs(seed, part) draws one part's arguments, and reference() takes and returns one part's arrays. A program takes and returns all parts, laid end to end along the dimension named above; an argument that names none is the same for every part. Nothing has to cross between parts.
Inputs may be any that keep to these rules, and one draw needn't show every extreme that they name: `edge_slot`: on each device, the live slots name every entry of its 16 * 16 list at least once, or as many distinct entries as there are live slots where these are fewer. `edge_count`: the counts sum to 16 * 2048 and one device has all 4096 slots live.
All inputs are finite; a program needn't handle non-finite values.
Results may differ from the reference program's by a relative error of at most 0.0071.
Values may be sent and summed in bfloat16 or wider, within the bound.
A program may use at most 64 MiB of HBM per device.

```python
import jax
import jax.numpy as jnp
from jax import lax

LAT = 512
VARS = 84
G_DEV = 1024
M_DEV = 640
E_DEV = 4096
CAP = 16
STEPS = 20
FREQ = 16
C_COND = 168
C_RAW = 252
GRID = 16384
MESH = 10240
EDGES = 65536
PAIRS = 256
N_NODE = 16


def live_counts(key):
    base_key = jax.random.fold_in(key, 11)
    order_key, spread_key = jax.random.split(base_key)
    order = jax.random.permutation(order_key, N_NODE).astype(jnp.int32)
    position = jnp.arange(N_NODE, dtype=jnp.int32)
    others = N_NODE - 1
    excess = E_DEV // 2
    share = excess // others
    remain = excess % others
    loss = share + (position - 1 < remain).astype(jnp.int32)
    spread = jax.random.randint(spread_key, (N_NODE,), 0, E_DEV // 8 + 1).astype(jnp.int32)
    following = jnp.where(position == N_NODE - 1, 1, position + 1).astype(jnp.int32)
    delta = spread - spread[following]
    placed = jnp.where(position == 0, E_DEV, E_DEV // 2 - loss + delta).astype(jnp.int32)
    return jnp.zeros((N_NODE,), jnp.int32).at[order].set(placed)


def draw_edge_count(key, part):
    return live_counts(key)


def draw_edge_slot(key, part):
    counts = live_counts(key)
    listed = N_NODE * CAP
    slot_key = jax.random.fold_in(key, 23)
    device_keys = jax.vmap(lambda index: jax.random.fold_in(slot_key, index))(jnp.arange(N_NODE, dtype=jnp.int32))

    def one_device(device_key, count):
        first_key, second_key = jax.random.split(device_key)
        order = jax.random.permutation(first_key, listed).astype(jnp.int32)
        extra = jax.random.randint(second_key, (E_DEV,), 0, listed).astype(jnp.int32)
        used = jnp.minimum(count, listed)
        position = jnp.arange(E_DEV, dtype=jnp.int32)
        pick = jnp.where(position < listed, position, extra % used)
        pick = jnp.minimum(pick, listed - 1)
        return order[pick]
    return jax.vmap(one_device)(device_keys, counts).reshape(N_NODE * E_DEV)


def plant(drawn, stream_key, smallest, high):
    longest = drawn.shape.index(max(drawn.shape))
    spots = []
    for shift in (0, 1):
        where = [jax.random.randint(jax.random.fold_in(stream_key, axis), (), 0, length) for axis, length in enumerate(drawn.shape)]
        where[longest] = (where[longest] + shift) % drawn.shape[longest]
        spots.append(tuple(where))
    return drawn.at[spots[0]].set(smallest).at[spots[1]].set(high)


def block_levels(key, shape, shards, least, largest):
    factor_of, own = 1.0, jax.random.fold_in(key, 6)
    for axis_at, blocks in shards:
        steps = jnp.exp(jax.random.uniform(jax.random.fold_in(own, axis_at), (blocks,), jnp.float32, least / len(shards), largest / len(shards)))
        factor_of = factor_of * jnp.repeat(steps, shape[axis_at] // blocks).reshape([-1 if axis == axis_at else 1 for axis in range(len(shape))])
    return factor_of


def gaussian(key, extent, width, limit, pieces=(), held_as=jnp.bfloat16):
    drawn = width * jax.random.normal(key, extent, jnp.float32)
    if pieces:
        drawn = drawn * block_levels(key, extent, pieces, -0.22, 0.18)
    return jnp.clip(drawn, -limit, limit).astype(held_as)


def setup_inputs(seed: int = 0, part: int = 0) -> dict:
    arg_keys = jax.random.split(jax.random.key(seed), 22)
    part_splits = jax.random.split(jax.random.fold_in(arg_keys[21], part), 22)
    return {
        "conditioning": gaussian(part_splits[0], (C_COND, GRID), 1.0, 6.0, ((1, 16),)),
        "target_state": gaussian(part_splits[1], (VARS, GRID), 1.0, 6.0, ((1, 16),), jnp.float32),
        "noise_sample": gaussian(part_splits[2], (VARS, GRID), 1.0, 6.0, ((1, 16),), jnp.float32),
        "step_index": jax.random.randint(part_splits[3], (1,), 0, STEPS).astype(jnp.int32),
        "mesh_features": jnp.clip(jax.random.uniform(arg_keys[4], (3, MESH), jnp.float32, -1.0, 1.0) * block_levels(arg_keys[4], (3, MESH), ((1, 16),), -0.4, 0.0), -1.0, 1.0),
        "edge_geometry": gaussian(arg_keys[5], (4, EDGES), 1.0, 6.0, ((1, 16),), jnp.float32),
        "edge_slot": draw_edge_slot(jax.random.fold_in(arg_keys[21], 71), part),
        "edge_receiver": plant(jax.random.randint(arg_keys[7], (EDGES,), 0, M_DEV), jax.random.fold_in(arg_keys[7], 1), 0, M_DEV - 1).astype(jnp.int32),
        "send_rows": plant(jax.random.randint(arg_keys[8], (PAIRS, CAP), 0, G_DEV), jax.random.fold_in(arg_keys[8], 1), 0, G_DEV - 1).astype(jnp.int32),
        "edge_count": draw_edge_count(jax.random.fold_in(arg_keys[21], 71), part),
        "embed_weight": gaussian(arg_keys[10], (C_RAW, LAT), C_RAW ** -0.5, 0.375),
        "mesh_weight": gaussian(arg_keys[11], (3, LAT), 3 ** -0.5, 3.5, (), jnp.float32),
        "geom_weight": gaussian(arg_keys[12], (4, LAT), 4 ** -0.5, 3.0, (), jnp.float32),
        "sender_weight": gaussian(arg_keys[13], (LAT, LAT), (3 * LAT) ** -0.5, 0.15625, ((0, 16),)),
        "edge_weight": gaussian(arg_keys[14], (LAT, LAT), (3 * LAT) ** -0.5, 0.15625, ((0, 16),)),
        "receiver_weight": gaussian(arg_keys[15], (LAT, LAT), (3 * LAT) ** -0.5, 0.15625, ((0, 16),)),
        "message_weight": gaussian(arg_keys[16], (LAT, LAT), LAT ** -0.5, 0.25, ((0, 16),)),
        "node_weight": gaussian(arg_keys[17], (2 * LAT, LAT), (2 * LAT) ** -0.5, 0.1875, ((0, 16),)),
        "output_weight": gaussian(arg_keys[18], (LAT, LAT), LAT ** -0.5, 0.25, ((0, 16),)),
        "noise_weight": gaussian(arg_keys[19], (2 * FREQ, LAT), (2 * FREQ) ** -0.5, 1.0, (), jnp.float32),
        "film_weight": gaussian(arg_keys[20], (LAT, 4 * LAT), LAT ** -0.5, 0.25),
    }


sigma_top = 80.0
sigma_low = 0.03
rho_power = 7.0
norm_eps = 1e-05

def layer_norm(values):
    mean = lax.optimization_barrier(jnp.mean(values, axis=-1, keepdims=True))
    centred = values - mean
    var = lax.optimization_barrier(jnp.mean(centred * centred, axis=-1, keepdims=True))
    return centred * lax.rsqrt(var + norm_eps)

def noise_terms(step_index, noise_weight, film_weight):
    frac = step_index[0].astype(jnp.float32) / (STEPS - 1)
    upper = sigma_top ** (1.0 / rho_power)
    lower = sigma_low ** (1.0 / rho_power)
    sigma = (upper + frac * (lower - upper)) ** rho_power
    angle = 0.25 * jnp.log(sigma) * (jnp.arange(FREQ, dtype=jnp.float32) + 1.0)
    fourier = jnp.concatenate([jnp.sin(angle), jnp.cos(angle)])[None, :]
    cond = jax.nn.silu(jnp.dot(fourier, noise_weight, precision=lax.Precision.HIGHEST)).astype(jnp.bfloat16)
    film = jnp.dot(cond, film_weight, preferred_element_type=jnp.float32)
    return (sigma, film)

def reference(conditioning, target_state, noise_sample, step_index, mesh_features, edge_geometry, edge_slot, edge_receiver, send_rows, edge_count, embed_weight, mesh_weight, geom_weight, sender_weight, edge_weight, receiver_weight, message_weight, node_weight, output_weight, noise_weight, film_weight):
    sigma, film = noise_terms(step_index, noise_weight, film_weight)
    edge_scale = film[:, 0:LAT]
    edge_shift = film[:, LAT:2 * LAT]
    node_scale = film[:, 2 * LAT:3 * LAT]
    node_shift = film[:, 3 * LAT:4 * LAT]
    noisy = ((target_state + sigma * noise_sample) / jnp.sqrt(sigma * sigma + 1.0)).astype(jnp.bfloat16)
    raw = jnp.concatenate([conditioning, noisy], axis=0)
    grid_latent = jax.nn.silu(jnp.dot(raw.T, embed_weight, preferred_element_type=jnp.float32)).astype(jnp.bfloat16)
    mesh_embed = jax.nn.silu(jnp.dot(mesh_features.T, mesh_weight, precision=lax.Precision.HIGHEST)).astype(jnp.bfloat16)
    recv_proj = jnp.dot(mesh_embed, receiver_weight, preferred_element_type=jnp.float32).astype(jnp.bfloat16)
    edge_embed = jax.nn.silu(jnp.dot(edge_geometry.T, geom_weight, precision=lax.Precision.HIGHEST)).astype(jnp.bfloat16)
    tables = send_rows.reshape(N_NODE, N_NODE, CAP)
    bands = jnp.arange(N_NODE, dtype=jnp.int32)

    def one_device(device):
        table = lax.dynamic_index_in_dim(tables, device, 1, keepdims=False)
        grid_index = (bands[:, None] * G_DEV + table).reshape(N_NODE * CAP)
        start = (device * E_DEV).astype(jnp.int32)
        slots = lax.dynamic_slice_in_dim(edge_slot, start, E_DEV, 0)
        local_recv = lax.dynamic_slice_in_dim(edge_receiver, start, E_DEV, 0)
        embed_rows = lax.dynamic_slice_in_dim(edge_embed, start, E_DEV, 0)
        node_start = (device * M_DEV).astype(jnp.int32)
        proj_local = lax.dynamic_slice_in_dim(recv_proj, node_start, M_DEV, 0)
        mesh_local = lax.dynamic_slice_in_dim(mesh_embed, node_start, M_DEV, 0)
        sender_rows = grid_latent[grid_index[slots]]
        pre = jnp.dot(embed_rows, edge_weight, preferred_element_type=jnp.float32)
        pre = pre + jnp.dot(sender_rows, sender_weight, preferred_element_type=jnp.float32)
        pre = pre + proj_local[local_recv].astype(jnp.float32)
        hidden = jax.nn.silu(pre).astype(jnp.bfloat16)
        mixed = jnp.dot(hidden, message_weight, preferred_element_type=jnp.float32)
        message = layer_norm(mixed) * (1.0 + edge_scale) + edge_shift
        count = lax.dynamic_index_in_dim(edge_count, device, 0, keepdims=False)
        live = jnp.arange(E_DEV, dtype=jnp.int32) < count
        message = jnp.where(live[:, None], message, 0.0).astype(jnp.bfloat16)
        gathered = jax.ops.segment_sum(message.astype(jnp.float32), local_recv, num_segments=M_DEV).astype(jnp.bfloat16)
        joined = jnp.concatenate([mesh_local, gathered], axis=1)
        update = jax.nn.silu(jnp.dot(joined, node_weight, preferred_element_type=jnp.float32)).astype(jnp.bfloat16)
        result = jnp.dot(update, output_weight, preferred_element_type=jnp.float32)
        return (mesh_local.astype(jnp.float32) + layer_norm(result) * (1.0 + node_scale) + node_shift).astype(jnp.bfloat16)
    blocks = lax.map(one_device, bands)
    return blocks.reshape(MESH, LAT)
```

```python
import functools

import jax
import jax.numpy as jnp
from jax import lax
from jax.experimental import pallas as pl
from jax.experimental.pallas import tpu as pltpu
from jax.sharding import PartitionSpec as P

STEPS = 20


sigma_top = 80.0
sigma_low = 0.03
rho_power = 7.0
norm_eps = 1e-05
f32, bf16 = jnp.float32, jnp.bfloat16


def is_folded(mesh):
    rows = mesh.devices[0]
    places = [getattr(device, "coords", None) for device in rows[:5:2]]
    if len(places) < 3 or any(place is None for place in places):
        return False
    first = [a != b for a, b in zip(places[0], places[1])]
    second = [a != b for a, b in zip(places[0], places[2])]
    return first != second


def silu(x):
    half = 0.5 * x
    return half * jnp.tanh(half) + half


def normalised(values):
    mean = jnp.mean(values, axis=1, keepdims=True)
    centred = values - mean
    var = jnp.mean(centred * centred, axis=1, keepdims=True)
    return centred * lax.rsqrt(var + norm_eps)


def nn(a, b):
    return jnp.dot(a, b, preferred_element_type=f32)


def nt(a, b):
    return lax.dot_general(a, b, (((1,), (1,)), ((), ())), preferred_element_type=f32)


def pieces(values):
    high = values.astype(bf16).astype(f32)
    rest = values - high
    middle = rest.astype(bf16).astype(f32)
    low = (rest - middle).astype(bf16).astype(f32)
    return high, middle, low


def stack_left(ref, values):
    a, b, c = pieces(values)
    ref[...] = jnp.zeros_like(ref)
    for i, part in enumerate((a, a, b, a, c, b)):
        ref[8 * i : 8 * i + values.shape[0], :] = part


def stack_right(ref, values):
    a, b, c = pieces(values)
    ref[...] = jnp.zeros_like(ref)
    for i, part in enumerate((a, b, a, c, a, b)):
        ref[8 * i : 8 * i + values.shape[0], :] = part


def encoder_kernel(n, members, folded, block, *refs):
    step_ref, count_ref = refs[:2]
    sources, shards, out_ref = refs[2:15], refs[15:21], refs[21]
    locals_, refs = refs[22:35], refs[35:]
    slot_ref, recv_ref, rows_ref, geom_ref, mesh_ref = locals_[:5]
    cond_ref, target_ref, noise_ref, embed_ref, mesh_w_ref, geom_w_ref, noise_w_ref, film_w_ref = locals_[5:]
    w_ref, raw_ref, pick_ref, outgoing, arrived, embed_pad_ref, turn_ref = refs[:7]
    mesh_s_ref, mesh_k_ref, geom_s_ref, geom_k_ref, nodes_ref, ohr_ref, ohs_ref = refs[7:14]
    place_ref, meshg_ref, edges_ref, pre_ref, table_ref, mixed_ref, total_ref = refs[14:21]
    z_send, z_recv, y_send, y_recv, x_send, x_recv, c_send, c_recv = refs[21:29]
    a_send, a_recv, in_sem, own_sem = refs[29:]
    me = lax.axis_index("node")
    member = lax.axis_index("member")
    wide = 2 if folded else 1
    deep = n // 2 // wide
    core, chip = me % 2, me // 2
    y, z = chip % wide, chip // wide
    paired = members % 2 == 0
    x = member % 2 if paired else 0
    other_member = member + 1 - 2 * x
    width = w_ref.shape[3]
    part = width // 2 if paired else width

    def node_at(zz, yy, cc):
        return (zz * wide + yy) * 2 + cc

    sent = []

    def remote(source, target, send, recv, device):
        copy = pltpu.make_async_remote_copy(
            src_ref=source, dst_ref=target, send_sem=send, recv_sem=recv, device_id=device
        )
        copy.start()
        sent.append(copy)
        return copy

    barrier = pltpu.get_barrier_semaphore()
    for step in range(1, n):
        pl.semaphore_signal(barrier, inc=1, device_id={"node": (me + step) % n})
    if paired:
        pl.semaphore_signal(barrier, inc=1, device_id={"member": other_member})
    loads = []
    for i, (source, target) in enumerate(zip(sources, locals_)):
        loads.append(pltpu.make_async_copy(source, target, in_sem.at[i]))

    def load(*which):
        for i in which:
            loads[i].start()

    def ready(*which):
        for i in which:
            loads[i].wait()

    load(2, 5, 6, 7)
    offsets, own = [0], []
    mine = y * 2 + core
    for k, shard in enumerate(shards):
        rows = shard.shape[0]
        target = w_ref.at[z, mine, pl.ds(offsets[k], rows), :]
        own.append(pltpu.make_async_copy(shard, target, own_sem.at[k]))
        own[k].start()
        offsets.append(offsets[k] + rows)
    load(0, 1, 3, 4, 9, 10, 8, 11, 12)

    groups = [(offsets[0], offsets[1]), (offsets[1], offsets[3]), (offsets[3], offsets[4]), (offsets[4], offsets[6])]
    near = x * part
    away = (1 - x) * part if paired else 0
    flights = {}

    def region(zz, lane, g, side):
        start, stop = groups[g]
        columns = pl.ds(pl.multiple_of(side, 128), part)
        return w_ref.at[zz, lane, pl.ds(start, stop - start), columns]

    def pass_core(g, i, zz, lane, side):
        spot = region(zz, lane, g, side)
        flights["c", g, i] = remote(spot, spot, c_send.at[g, i], c_recv.at[g, i], {"node": me + 1 - 2 * core})

    def pass_member(g, i, zz, lane):
        spot = region(zz, lane, g, near)
        flights["x", g, i] = remote(spot, spot, x_send.at[g, i], x_recv.at[g, i], {"member": other_member})

    def start_z(g):
        for j in range(1, deep):
            spot = region(z, mine, g, near)
            device = {"node": node_at((z + j) % deep, y, core)}
            flights["z", g, j] = remote(spot, spot, z_send.at[g, j], z_recv.at[g, j], device)

    every = pl.ds(0, deep)
    facing = (1 - y) * 2 + core

    def step_y(g):
        for j in range(1, deep):
            flights["z", g, j].wait_recv()
        if wide == 2:
            spot = region(every, mine, g, near)
            device = {"node": node_at(z, 1 - y, core)}
            flights["y", g] = remote(spot, spot, y_send.at[g], y_recv.at[g], device)
        if paired:
            for j in range(1, deep):
                pass_member(g, j, (z + j) % deep, mine)
        pass_core(g, 0, every, mine, near)

    def step_x(g):
        if wide == 2:
            flights["y", g].wait_recv()
            if paired:
                pass_member(g, 0, every, facing)
            pass_core(g, 1, every, facing, near)

    def step_c(g):
        if paired:
            for j in range(1, deep):
                flights["x", g, j].wait_recv()
            pass_core(g, 2, every, mine, away)
            if wide == 2:
                flights["x", g, 0].wait_recv()
                pass_core(g, 3, every, facing, away)

    def step_in(g):
        for i in range(4):
            if ("c", g, i) in flights:
                flights["c", g, i].wait_recv()

    def weight(k):
        return w_ref[:, :, offsets[k] : offsets[k + 1], :].reshape(-1, width)

    channels = embed_ref.shape[0]
    cap = rows_ref.shape[1]
    listed = n * cap
    points, fixed = cond_ref.shape[1], cond_ref.shape[0]
    frac = jnp.full((1, 1), step_ref[0], jnp.int32).astype(f32) / (STEPS - 1)
    upper = sigma_top ** (1.0 / rho_power)
    lower = sigma_low ** (1.0 / rho_power)
    root = upper + frac * (lower - upper)
    cube = root * root * root
    sigma = cube * cube * root
    turn_ref[...] = jnp.zeros_like(turn_ref)
    raw_ref[...] = jnp.zeros_like(raw_ref)
    ready(2)
    turn_ref[:n, :cap] = rows_ref[...].astype(f32)
    turned = turn_ref[...].T
    spots = lax.broadcasted_iota(jnp.int32, (cap, points), 1).astype(f32)
    for r in range(n):
        chosen = turned[:cap, r : r + 1] == spots
        pick_ref[r * cap : (r + 1) * cap, :] = chosen.astype(f32).astype(bf16)
    ready(5, 6, 7)
    raw_ref[:fixed, :] = cond_ref[...].astype(f32)
    raw_ref[fixed:channels, :] = (target_ref[...] + sigma * noise_ref[...]) / jnp.sqrt(sigma * sigma + 1.0)
    outgoing[...] = nt(pick_ref[...], raw_ref[...].astype(bf16)).astype(bf16).reshape(outgoing.shape)

    ready(4, 9)
    stack_left(mesh_s_ref, mesh_ref[...])
    stack_right(mesh_k_ref, mesh_w_ref[...])
    nodes_ref[...] = silu(nn(mesh_s_ref[...].T.astype(bf16), mesh_k_ref[...].astype(bf16))).astype(bf16)
    ready(3, 10)
    stack_left(geom_s_ref, geom_ref[...])
    stack_right(geom_k_ref, geom_w_ref[...])
    ready(0, 1)
    count = count_ref[0]
    nodes = mesh_ref.shape[1]
    blocks = geom_ref.shape[1] // block
    chunks = block // 128
    lanes = lax.broadcasted_iota(jnp.int32, (128, 128), 1).astype(f32)
    lane_row = lax.broadcasted_iota(jnp.int32, (1, 128), 1)
    node_rows = lax.broadcasted_iota(jnp.int32, (nodes, 128), 0).astype(f32)

    def prepare(b, carry):
        for c in range(chunks):
            j = b * chunks + c
            here = pl.ds(c * 128, 128)
            from_row = slot_ref[pl.ds(j, 1), :].astype(f32)
            to_row = jnp.where(j * 128 + lane_row < count, recv_ref[pl.ds(j, 1), :], -1).astype(f32)
            from_cols = jnp.broadcast_to(from_row, (128, 128)).T
            to_cols = jnp.broadcast_to(to_row, (128, 128)).T
            for t in range(listed // 128):
                ohs_ref[b, here, t * 128 : (t + 1) * 128] = (from_cols == lanes + 128.0 * t).astype(f32).astype(bf16)
            for t in range(nodes // 128):
                ohr_ref[here, t * 128 : (t + 1) * 128] = (to_cols == lanes + 128.0 * t).astype(f32).astype(bf16)
            place_ref[b, :, here] = (node_rows == to_row).astype(f32).astype(bf16)
        meshg_ref[b] = nn(ohr_ref[...], nodes_ref[...]).astype(bf16)
        here = pl.ds(pl.multiple_of(b * block, block), block)
        embedded = nn(geom_s_ref[:, here].T.astype(bf16), geom_k_ref[...].astype(bf16))
        edges_ref[b] = silu(embedded).astype(bf16)
        return carry

    def prepare_to(start, stop):
        lax.fori_loop(blocks * start // 8, blocks * stop // 8, prepare, 0)

    for copy in own:
        copy.wait()
    prepare_to(0, 2)
    pl.semaphore_wait(barrier, n if paired else n - 1)
    start_z(0)
    start_z(1)
    swaps = []
    for step in range(1, n):
        other = (me + step) % n
        swaps.append(
            remote(outgoing.at[other], arrived.at[me], a_send.at[step], a_recv.at[step], {"node": other})
        )
    start_z(2)
    start_z(3)
    stay = pltpu.make_async_copy(outgoing.at[me], arrived.at[me], own_sem.at[6])
    stay.start()
    prepare_to(2, 5)
    step_y(0)
    prepare_to(5, 6)
    step_y(1)
    step_x(0)
    prepare_to(6, 7)
    step_y(2)
    step_x(1)
    prepare_to(7, 8)
    step_c(0)
    step_x(2)

    ready(8, 11, 12)
    embed_pad_ref[...] = jnp.zeros_like(embed_pad_ref)
    embed_pad_ref[:channels, :] = embed_ref[...]
    freqs = noise_w_ref.shape[0] // 2
    place_k = lax.broadcasted_iota(jnp.int32, (2 * freqs, 1), 0)
    wave = (place_k % freqs + 1).astype(f32)
    angle = 0.25 * jnp.log(sigma) * wave
    fourier = jnp.where(place_k < freqs, jnp.sin(angle), jnp.cos(angle))
    cond = silu(jnp.sum(fourier * noise_w_ref[...], axis=0, keepdims=True)).astype(bf16)
    film = nn(cond, film_w_ref[...])
    edge_scale, edge_shift, node_scale, node_shift = [film[:, width * i : width * (i + 1)] for i in range(4)]
    stay.wait()
    for copy in swaps:
        copy.wait_recv()
    listing = arrived[...].reshape(listed, arrived.shape[2])
    received = silu(nn(listing, embed_pad_ref[...])).astype(bf16)
    step_c(1)
    step_in(0)

    def edge_part(i, carry):
        for u in range(2):
            pre_ref[2 * i + u] = nn(edges_ref[2 * i + u], weight(0))
        return carry

    lax.fori_loop(0, blocks // 4, edge_part, 0)
    step_c(2)
    step_y(3)
    step_in(1)
    lax.fori_loop(blocks // 4, blocks // 2, edge_part, 0)
    step_x(3)
    table_ref[...] = nn(received, weight(2)).astype(bf16)

    def hidden_part(i, carry):
        for u in range(2):
            b = 2 * i + u
            pre = pre_ref[b] + (nn(meshg_ref[b], weight(1)) + nn(ohs_ref[b], table_ref[...]))
            edges_ref[b] = silu(pre).astype(bf16)
        return carry

    lax.fori_loop(0, blocks // 2, hidden_part, 0)
    step_c(3)
    step_in(2)
    total_ref[...] = jnp.zeros_like(total_ref)
    mixed_ref[0] = nn(edges_ref[0], weight(3))
    for b in range(blocks):
        if b + 1 < blocks:
            mixed_ref[(b + 1) % 2] = nn(edges_ref[b + 1], weight(3))
        message = normalised(mixed_ref[b % 2]) * (1.0 + edge_scale) + edge_shift
        total_ref[...] += nn(place_ref[b], message.astype(bf16))
    step_in(3)
    joint = weight(5)
    update = nn(nodes_ref[...], joint[:width]) + nn(total_ref[...].astype(bf16), joint[width:])
    update = silu(update).astype(bf16)
    result = normalised(nn(update, weight(4))) * (1.0 + node_scale) + node_shift
    out_ref[...] = (nodes_ref[...].astype(f32) + result).astype(bf16)
    for copy in sent:
        copy.wait_send()


def per_device(n, members, folded, *args):
    conditioning, target_state, noise_sample, step_index, mesh_features, edge_geometry = args[:6]
    edge_slot, edge_receiver, send_rows, edge_count, embed_weight, mesh_weight, geom_weight = args[6:13]
    sender_w, edge_w, receiver_w, message_w, node_w, output_w = args[13:19]
    noise_weight, film_weight = args[19:]
    shards = (edge_w, receiver_w, sender_w, message_w, output_w, node_w)
    channels, width = embed_weight.shape
    nodes, edges = mesh_features.shape[1], edge_geometry.shape[1]
    cap = send_rows.shape[1]
    points = conditioning.shape[1]
    listed = n * cap
    deep = channels + -channels % 128
    block = min(512, edges)
    blocks = edges // block
    lines = 2 if folded else 1
    layers = n // 2 // lines
    stacked = sum(shard.shape[0] for shard in shards)
    inputs = (
        edge_slot.reshape(-1, 128),
        edge_receiver.reshape(-1, 128),
        send_rows,
        edge_geometry,
        mesh_features,
        conditioning,
        target_state,
        noise_sample,
        embed_weight,
        mesh_weight,
        geom_weight,
        noise_weight,
        film_weight,
    )
    dma = pltpu.SemaphoreType.DMA
    vmem = pl.BlockSpec(memory_space=pltpu.VMEM)
    smem = pl.BlockSpec(memory_space=pltpu.SMEM)
    hbm = pl.BlockSpec(memory_space=pltpu.HBM)
    return pl.pallas_call(
        functools.partial(encoder_kernel, n, members, folded, block),
        out_shape=jax.ShapeDtypeStruct((nodes, width), bf16),
        in_specs=[smem] * 2 + [hbm] * 19,
        out_specs=vmem,
        scratch_shapes=[pltpu.VMEM(value.shape, value.dtype) for value in inputs]
        + [
            pltpu.VMEM((layers, 2 * lines, stacked, width), bf16),
            pltpu.VMEM((deep, points), f32),
            pltpu.VMEM((listed, points), bf16),
            pltpu.VMEM((n, cap, deep), bf16),
            pltpu.VMEM((n, cap, deep), bf16),
            pltpu.VMEM((deep, width), bf16),
            pltpu.VMEM((128, 128), f32),
            pltpu.VMEM((128, nodes), f32),
            pltpu.VMEM((128, width), f32),
            pltpu.VMEM((128, edges), f32),
            pltpu.VMEM((128, width), f32),
            pltpu.VMEM((nodes, width), bf16),
            pltpu.VMEM((block, nodes), bf16),
            pltpu.VMEM((blocks, block, listed), bf16),
            pltpu.VMEM((blocks, nodes, block), bf16),
            pltpu.VMEM((blocks, block, width), bf16),
            pltpu.VMEM((blocks, block, width), bf16),
            pltpu.VMEM((blocks, block, width), f32),
            pltpu.VMEM((listed, width), bf16),
            pltpu.VMEM((2, block, width), f32),
            pltpu.VMEM((nodes, width), f32),
            dma((4, layers)),
            dma((4, layers)),
            dma((4,)),
            dma((4,)),
            dma((4, layers)),
            dma((4, layers)),
            dma((4, 4)),
            dma((4, 4)),
            dma((n,)),
            dma((n,)),
            dma((13,)),
            dma((7,)),
        ],
        compiler_params=pltpu.CompilerParams(
            collective_id=0, has_side_effects=True, vmem_limit_bytes=48 * 1024 * 1024
        ),
    )(step_index, edge_count, *inputs, *shards)


def solution(mesh):
    placed = (
        P(None, ("member", "node")),
        P(None, ("member", "node")),
        P(None, ("member", "node")),
        P("member"),
        P(None, "node"),
        P(None, "node"),
        P("node"),
        P("node"),
        P("node", None),
        P("node"),
        P(),
        P(),
        P(),
        P("node", None),
        P("node", None),
        P("node", None),
        P("node", None),
        P("node", None),
        P("node", None),
        P(),
        P(),
    )
    body = functools.partial(per_device, mesh.shape["node"], mesh.shape["member"], is_folded(mesh))
    return jax.shard_map(
        body, mesh=mesh, in_specs=placed, out_specs=P("node", "member"), check_vma=False
    )
```

```python
import functools

import jax
import jax.numpy as jnp
from jax import lax
from jax.experimental import pallas as pl
from jax.experimental.pallas import tpu as pltpu
from jax.sharding import PartitionSpec as P

STEPS = 20


sigma_top = 80.0
sigma_low = 0.03
rho_power = 7.0
norm_eps = 1e-05
f32, bf16 = jnp.float32, jnp.bfloat16


def is_folded(mesh):
    rows = mesh.devices[0]
    places = [getattr(device, "coords", None) for device in rows[:5:2]]
    if len(places) < 3 or any(place is None for place in places):
        return False
    first = [a != b for a, b in zip(places[0], places[1])]
    second = [a != b for a, b in zip(places[0], places[2])]
    return first != second


def silu(x):
    half = 0.5 * x
    return half * jnp.tanh(half) + half


def normalised(values):
    mean = jnp.mean(values, axis=1, keepdims=True)
    centred = values - mean
    var = jnp.mean(centred * centred, axis=1, keepdims=True)
    return centred * lax.rsqrt(var + norm_eps)


def nn(a, b):
    return jnp.dot(a, b, preferred_element_type=f32)


def nt(a, b):
    return lax.dot_general(a, b, (((1,), (1,)), ((), ())), preferred_element_type=f32)


def pieces(values):
    high = values.astype(bf16).astype(f32)
    rest = values - high
    middle = rest.astype(bf16).astype(f32)
    low = (rest - middle).astype(bf16).astype(f32)
    return high, middle, low


def stack_left(ref, values):
    a, b, c = pieces(values)
    ref[...] = jnp.zeros_like(ref)
    for i, part in enumerate((a, a, b, a, c, b)):
        ref[8 * i : 8 * i + values.shape[0], :] = part


def stack_right(ref, values):
    a, b, c = pieces(values)
    ref[...] = jnp.zeros_like(ref)
    for i, part in enumerate((a, b, a, c, a, b)):
        ref[8 * i : 8 * i + values.shape[0], :] = part


def encoder_kernel(n, members, folded, block, *refs):
    step_ref, count_ref = refs[:2]
    sources, shards, out_ref = refs[2:15], refs[15:21], refs[21]
    locals_, refs = refs[22:35], refs[35:]
    slot_ref, recv_ref, rows_ref, geom_ref, mesh_ref = locals_[:5]
    cond_ref, target_ref, noise_ref, embed_ref, mesh_w_ref, geom_w_ref, noise_w_ref, film_w_ref = locals_[5:]
    w_ref, raw_ref, pick_ref, outgoing, arrived, embed_pad_ref, turn_ref = refs[:7]
    mesh_s_ref, mesh_k_ref, geom_s_ref, geom_k_ref, nodes_ref, ohr_ref, ohs_ref = refs[7:14]
    place_ref, meshg_ref, edges_ref, pre_ref, table_ref, mixed_ref, total_ref = refs[14:21]
    film_ref, received_ref = refs[21:23]
    z_recv, y_recv, x_recv, f_recv, c_recv, a_recv, sent_sem, in_sem, own_sem, heard = refs[23:]
    me = lax.axis_index("node")
    member = lax.axis_index("member")
    wide = 2 if folded else 1
    deep = n // 2 // wide
    core, chip = me % 2, me // 2
    y, z = chip % wide, chip // wide
    paired = members % 2 == 0
    x = member % 2 if paired else 0
    other_member = member + 1 - 2 * x
    width = w_ref.shape[3]
    part = width // 2 if paired else width

    def node_at(zz, yy, cc):
        return (zz * wide + yy) * 2 + cc

    def remote(source, target, way, recv, device):
        copy = pltpu.make_async_remote_copy(
            src_ref=source, dst_ref=target, send_sem=sent_sem.at[way], recv_sem=recv, device_id=device
        )
        copy.start()

    def arrive(like, sem):
        pltpu.make_async_copy(like, like, sem).wait()

    barrier = pltpu.get_barrier_semaphore()
    greeted = [{"node": node_at((z + j) % deep, y, core)} for j in range(1, deep)]
    greeted.append({"node": me + 1 - 2 * core})
    if wide == 2:
        greeted.append({"node": node_at(z, 1 - y, core)})
    if paired:
        greeted.append({"member": other_member})
    for device in greeted:
        pl.semaphore_signal(barrier, inc=1, device_id=device)
    loads = []
    for i, (source, target) in enumerate(zip(sources, locals_)):
        loads.append(pltpu.make_async_copy(source, target, in_sem.at[i]))

    def load(*which):
        for i in which:
            loads[i].start()

    def ready(*which):
        for i in which:
            loads[i].wait()

    load(2, 5, 6, 7)
    offsets = [0]
    mine = y * 2 + core
    for shard in shards:
        rows = shard.shape[0]
        target = w_ref.at[z, mine, pl.ds(offsets[-1], rows), :]
        pltpu.make_async_copy(shard, target, own_sem).start()
        offsets.append(offsets[-1] + rows)
    load(0, 1, 3, 4, 9, 10, 8, 11, 12)

    groups = [(offsets[k], offsets[k + 1]) for k in range(6)]
    near = x * part
    away = (1 - x) * part if paired else 0
    whole = ()
    every, others = pl.ds(0, deep), pl.ds(0, deep - 1)
    facing = (1 - y) * 2 + core
    partner = {"node": me + 1 - 2 * core}

    def halved(g):
        return paired and g not in whole

    def region(zz, lane, g, side):
        start, stop = groups[g]
        if not halved(g):
            return w_ref.at[zz, lane, pl.ds(start, stop - start), :]
        columns = pl.ds(pl.multiple_of(side, 128), part)
        return w_ref.at[zz, lane, pl.ds(start, stop - start), columns]

    def pass_core(g, lane, side):
        spot = region(every, lane, g, side)
        remote(spot, spot, 4, c_recv.at[g], partner)

    def start_z(g):
        for j in range(1, deep):
            spot = region(z, mine, g, near)
            remote(spot, spot, 0, z_recv.at[g], {"node": node_at((z + j) % deep, y, core)})

    def step_y(g):
        arrive(region(others, mine, g, near), z_recv.at[g])
        if wide == 2:
            spot = region(every, mine, g, near)
            remote(spot, spot, 1, y_recv.at[g], {"node": node_at(z, 1 - y, core)})
        if halved(g):
            for j in range(1, deep):
                spot = region((z + j) % deep, mine, g, near)
                remote(spot, spot, 2, x_recv.at[g], {"member": other_member})
        pass_core(g, mine, near)

    def step_x(g):
        if wide == 2:
            spot = region(every, facing, g, near)
            arrive(spot, y_recv.at[g])
            if halved(g):
                remote(spot, spot, 3, f_recv.at[g], {"member": other_member})
            pass_core(g, facing, near)

    def step_c(g):
        if halved(g):
            arrive(region(others, mine, g, away), x_recv.at[g])
            pass_core(g, mine, away)
            if wide == 2:
                arrive(region(every, facing, g, away), f_recv.at[g])
                pass_core(g, facing, away)

    def step_in(g):
        start, stop = groups[g]
        arrive(w_ref.at[:, pl.ds(0, wide), pl.ds(start, stop - start), :], c_recv.at[g])

    def weight(k):
        return w_ref[:, :, offsets[k] : offsets[k + 1], :].reshape(-1, width)

    channels = embed_ref.shape[0]
    cap = rows_ref.shape[1]
    listed = n * cap
    points, fixed = cond_ref.shape[1], cond_ref.shape[0]
    frac = jnp.full((1, 1), step_ref[0], jnp.int32).astype(f32) / (STEPS - 1)
    upper = sigma_top ** (1.0 / rho_power)
    lower = sigma_low ** (1.0 / rho_power)
    root = upper + frac * (lower - upper)
    cube = root * root * root
    sigma = cube * cube * root
    def make_picks():
        turn_ref[...] = jnp.zeros_like(turn_ref)
        raw_ref[...] = jnp.zeros_like(raw_ref)
        ready(2)
        turn_ref[:n, :cap] = rows_ref[...].astype(f32)
        turned = turn_ref[...].T
        spots = lax.broadcasted_iota(jnp.int32, (cap, points), 1).astype(f32)
        for r in range(n):
            chosen = turned[:cap, r : r + 1] == spots
            pick_ref[r * cap : (r + 1) * cap, :] = chosen.astype(f32).astype(bf16)
        ready(5, 6, 7)
        raw_ref[:fixed, :] = cond_ref[...].astype(f32)
        raw_ref[fixed:channels, :] = (target_ref[...] + sigma * noise_ref[...]) / jnp.sqrt(sigma * sigma + 1.0)
        outgoing[...] = nt(pick_ref[...], raw_ref[...].astype(bf16)).astype(bf16).reshape(outgoing.shape)

    def make_nodes():
        ready(4, 9)
        stack_left(mesh_s_ref, mesh_ref[...])
        stack_right(mesh_k_ref, mesh_w_ref[...])
        nodes_ref[...] = silu(nn(mesh_s_ref[...].T.astype(bf16), mesh_k_ref[...].astype(bf16))).astype(bf16)
        ready(3, 10)
        stack_left(geom_s_ref, geom_ref[...])
        stack_right(geom_k_ref, geom_w_ref[...])
        ready(0, 1)

    count = count_ref[0]
    nodes = mesh_ref.shape[1]
    blocks = geom_ref.shape[1] // block
    chunks = block // 128
    lanes = lax.broadcasted_iota(jnp.int32, (128, 128), 1).astype(f32)
    lane_row = lax.broadcasted_iota(jnp.int32, (1, 128), 1)
    node_rows = lax.broadcasted_iota(jnp.int32, (nodes, 128), 0).astype(f32)

    def prepare(b, carry):
        for c in range(chunks):
            j = b * chunks + c
            here = pl.ds(c * 128, 128)
            from_row = slot_ref[pl.ds(j, 1), :].astype(f32)
            to_row = jnp.where(j * 128 + lane_row < count, recv_ref[pl.ds(j, 1), :], -1).astype(f32)
            from_cols = jnp.broadcast_to(from_row, (128, 128)).T
            to_cols = jnp.broadcast_to(to_row, (128, 128)).T
            for t in range(listed // 128):
                ohs_ref[b, here, t * 128 : (t + 1) * 128] = (from_cols == lanes + 128.0 * t).astype(f32).astype(bf16)
            for t in range(nodes // 128):
                ohr_ref[here, t * 128 : (t + 1) * 128] = (to_cols == lanes + 128.0 * t).astype(f32).astype(bf16)
            place_ref[b, :, here] = (node_rows == to_row).astype(f32).astype(bf16)
        meshg_ref[b] = nn(ohr_ref[...], nodes_ref[...]).astype(bf16)
        here = pl.ds(pl.multiple_of(b * block, block), block)
        embedded = nn(geom_s_ref[:, here].T.astype(bf16), geom_k_ref[...].astype(bf16))
        edges_ref[b] = silu(embedded).astype(bf16)
        return carry

    def prepare_to(start, stop):
        lax.fori_loop(blocks * start // 8, blocks * stop // 8, prepare, 0)

    def start_exchange():
        for step in range(1, n):
            other = (me + step) % n
            remote(outgoing.at[other], arrived.at[me], 5, a_recv, {"node": other})

    stay = pltpu.make_async_copy(outgoing.at[me], arrived.at[me], in_sem.at[2])

    def start_local(_, carry):
        make_picks()
        make_nodes()
        return carry

    def end_exchange():
        stay.wait()
        arrive(arrived.at[pl.ds(0, n - 1)], a_recv)

    def prepare_noise():
        ready(11, 12)
        freqs = noise_w_ref.shape[0] // 2
        place_k = lax.broadcasted_iota(jnp.int32, (2 * freqs, 1), 0)
        wave = (place_k % freqs + 1).astype(f32)
        angle = 0.25 * jnp.log(sigma) * wave
        fourier = jnp.where(place_k < freqs, jnp.sin(angle), jnp.cos(angle))
        cond = silu(jnp.sum(fourier * noise_w_ref[...], axis=0, keepdims=True)).astype(bf16)
        film = nn(cond, film_w_ref[...])
        film_ref[...] = film
        ready(8)
        embed_pad_ref[...] = jnp.zeros_like(embed_pad_ref)
        embed_pad_ref[:channels, :] = embed_ref[...]

    def receive():
        end_exchange()
        listing = arrived[...].reshape(listed, arrived.shape[2])
        received_ref[...] = silu(nn(listing, embed_pad_ref[...])).astype(bf16)

    def rows_of(b):
        return pl.ds(pl.multiple_of(b * block, block), block)

    def edge_part(b, carry):
        pre_ref[rows_of(b), :] = nn(edges_ref[b], weight(0))
        return carry

    def node_part(b, carry):
        pre_ref[rows_of(b), :] += nn(meshg_ref[b], weight(1))
        return carry

    def make_table():
        table_ref[...] = nn(received_ref[...], weight(2)).astype(bf16)

    def hidden_part(b, carry):
        pre = pre_ref[rows_of(b), :] + nn(ohs_ref[b], table_ref[...])
        edges_ref[b] = silu(pre).astype(bf16)
        return carry

    def film_row(k):
        return film_ref[:, width * k : width * (k + 1)]

    def mix(b):
        mixed_ref[b % 2] = nn(edges_ref[b], weight(3))

    def message_part(b):
        if b + 1 < blocks:
            mix(b + 1)
        message = normalised(mixed_ref[b % 2]) * (1.0 + film_row(0)) + film_row(1)
        total_ref[...] += nn(place_ref[b], message.astype(bf16))

    def loop(body, start, stop, unroll=2):
        first, last = blocks * start // 8, blocks * stop // 8
        unroll = min(unroll, last - first)
        if (last - first) % unroll:
            unroll = 1

        def several(i, carry):
            for u in range(unroll):
                body(first + unroll * i + u, carry)
            return carry

        lax.fori_loop(0, (last - first) // unroll, several, 0)

    arrive(w_ref.at[z, mine], own_sem)
    pl.semaphore_wait(barrier, len(greeted))
    pl.semaphore_signal(heard.at[0], inc=1, device_id=partner)
    start_z(0)
    start_z(1)
    start_z(2)
    start_z(3)
    pl.semaphore_wait(heard.at[0], 1)
    if wide == 2:
        pl.semaphore_signal(heard.at[1], inc=1, device_id={"node": node_at(z, 1 - y, core)})
    make_picks()
    if wide == 2:
        pl.semaphore_wait(heard.at[1], 1)
    start_exchange()
    stay.start()
    start_z(5)
    start_z(4)
    make_nodes()
    step_y(0)
    loop(prepare, 0, 1, 1)
    step_y(1)
    loop(prepare, 1, 2, 1)
    step_x(0)
    step_y(2)
    loop(prepare, 2, 3, 1)
    step_x(1)
    loop(prepare, 3, 4, 1)
    step_y(3)
    loop(prepare, 4, 5, 1)
    step_x(2)
    loop(prepare, 5, 6, 1)
    step_c(0)
    step_x(3)
    loop(prepare, 6, 7, 1)
    step_c(1)
    loop(prepare, 7, 8, 1)
    step_in(0)
    step_y(5)
    loop(edge_part, 0, 4, 8)
    step_c(2)
    loop(edge_part, 4, 8, 8)
    prepare_noise()
    step_in(1)
    loop(node_part, 0, 4, 8)
    step_c(3)
    step_x(5)
    loop(node_part, 4, 8, 8)
    receive()
    step_y(4)
    step_in(2)
    make_table()
    loop(hidden_part, 0, 4, 8)
    step_x(4)
    loop(hidden_part, 4, 8, 8)
    step_in(3)
    total_ref[...] = jnp.zeros_like(total_ref)
    mix(0)
    for b in range(blocks * 0 // 8, blocks * 2 // 8):
        message_part(b)
    step_c(5)
    for b in range(blocks * 2 // 8, blocks * 4 // 8):
        message_part(b)
    step_c(4)
    for b in range(blocks * 4 // 8, blocks * 8 // 8):
        message_part(b)
    step_in(5)
    step_in(4)
    joint = weight(5)
    update = nn(nodes_ref[...], joint[:width]) + nn(total_ref[...].astype(bf16), joint[width:])
    update = silu(update).astype(bf16)
    result = normalised(nn(update, weight(4))) * (1.0 + film_row(2)) + film_row(3)
    out_ref[...] = (nodes_ref[...].astype(f32) + result).astype(bf16)
    for g in range(6):
        arrive(region(others, mine, g, near), sent_sem.at[0])
        if wide == 2:
            arrive(region(every, mine, g, near), sent_sem.at[1])
        if halved(g):
            arrive(region(others, mine, g, near), sent_sem.at[2])
            if wide == 2:
                arrive(region(every, mine, g, near), sent_sem.at[3])
    arrive(w_ref.at[:, pl.ds(0, wide), :, :], sent_sem.at[4])
    arrive(arrived.at[pl.ds(0, n - 1)], sent_sem.at[5])


def per_device(n, members, folded, *args):
    conditioning, target_state, noise_sample, step_index, mesh_features, edge_geometry = args[:6]
    edge_slot, edge_receiver, send_rows, edge_count, embed_weight, mesh_weight, geom_weight = args[6:13]
    sender_w, edge_w, receiver_w, message_w, node_w, output_w = args[13:19]
    noise_weight, film_weight = args[19:]
    shards = (edge_w, receiver_w, sender_w, message_w, output_w, node_w)
    channels, width = embed_weight.shape
    nodes, edges = mesh_features.shape[1], edge_geometry.shape[1]
    cap = send_rows.shape[1]
    points = conditioning.shape[1]
    listed = n * cap
    deep = channels + -channels % 128
    block = min(512, edges)
    blocks = edges // block
    lines = 2 if folded else 1
    layers = n // 2 // lines
    stacked = sum(shard.shape[0] for shard in shards)
    inputs = (
        edge_slot.reshape(-1, 128),
        edge_receiver.reshape(-1, 128),
        send_rows,
        edge_geometry,
        mesh_features,
        conditioning,
        target_state,
        noise_sample,
        embed_weight,
        mesh_weight,
        geom_weight,
        noise_weight,
        film_weight,
    )
    dma = pltpu.SemaphoreType.DMA
    vmem = pl.BlockSpec(memory_space=pltpu.VMEM)
    smem = pl.BlockSpec(memory_space=pltpu.SMEM)
    hbm = pl.BlockSpec(memory_space=pltpu.HBM)
    return pl.pallas_call(
        functools.partial(encoder_kernel, n, members, folded, block),
        out_shape=jax.ShapeDtypeStruct((nodes, width), bf16),
        in_specs=[smem] * 2 + [hbm] * 19,
        out_specs=vmem,
        scratch_shapes=[pltpu.VMEM(value.shape, value.dtype) for value in inputs]
        + [
            pltpu.VMEM((layers, 2 * lines, stacked, width), bf16),
            pltpu.VMEM((deep, points), f32),
            pltpu.VMEM((listed, points), bf16),
            pltpu.VMEM((n, cap, deep), bf16),
            pltpu.VMEM((n, cap, deep), bf16),
            pltpu.VMEM((deep, width), bf16),
            pltpu.VMEM((128, 128), f32),
            pltpu.VMEM((128, nodes), f32),
            pltpu.VMEM((128, width), f32),
            pltpu.VMEM((128, edges), f32),
            pltpu.VMEM((128, width), f32),
            pltpu.VMEM((nodes, width), bf16),
            pltpu.VMEM((block, nodes), bf16),
            pltpu.VMEM((blocks, block, listed), bf16),
            pltpu.VMEM((blocks, nodes, block), bf16),
            pltpu.VMEM((blocks, block, width), bf16),
            pltpu.VMEM((blocks, block, width), bf16),
            pltpu.VMEM((edges, width), f32),
            pltpu.VMEM((listed, width), bf16),
            pltpu.VMEM((2, block, width), f32),
            pltpu.VMEM((nodes, width), f32),
            pltpu.VMEM((1, 4 * width), f32),
            pltpu.VMEM((listed, width), bf16),
            dma((6,)),
            dma((6,)),
            dma((6,)),
            dma((6,)),
            dma((6,)),
            dma,
            dma((6,)),
            dma((13,)),
            dma,
            pltpu.SemaphoreType.REGULAR((2,)),
        ],
        compiler_params=pltpu.CompilerParams(collective_id=0, has_side_effects=True),
    )(step_index, edge_count, *inputs, *shards)


def solution(mesh):
    placed = (
        P(None, ("member", "node")),
        P(None, ("member", "node")),
        P(None, ("member", "node")),
        P("member"),
        P(None, "node"),
        P(None, "node"),
        P("node"),
        P("node"),
        P("node", None),
        P("node"),
        P(),
        P(),
        P(),
        P("node", None),
        P("node", None),
        P("node", None),
        P("node", None),
        P("node", None),
        P("node", None),
        P(),
        P(),
    )
    body = functools.partial(per_device, mesh.shape["node"], mesh.shape["member"], is_folded(mesh))
    return jax.shard_map(
        body, mesh=mesh, in_specs=placed, out_specs=P("node", "member"), check_vma=False
    )
```

```python
import functools

import jax
import jax.numpy as jnp
from jax import lax
from jax.experimental import pallas as pl
from jax.experimental.pallas import tpu as pltpu
from jax.sharding import PartitionSpec as P

STEPS = 20


sigma_top = 80.0
sigma_low = 0.03
rho_power = 7.0
norm_eps = 1e-05
f32, bf16 = jnp.float32, jnp.bfloat16


def is_folded(mesh):
    rows = mesh.devices[0]
    places = [getattr(device, "coords", None) for device in rows[:5:2]]
    if len(places) < 3 or any(place is None for place in places):
        return False
    first = [a != b for a, b in zip(places[0], places[1])]
    second = [a != b for a, b in zip(places[0], places[2])]
    return first != second


def silu(x):
    half = 0.5 * x
    return half * jnp.tanh(half) + half


def normalised(values):
    mean = jnp.mean(values, axis=1, keepdims=True)
    centred = values - mean
    var = jnp.mean(centred * centred, axis=1, keepdims=True)
    return centred * lax.rsqrt(var + norm_eps)


def nn(a, b):
    return jnp.dot(a, b, preferred_element_type=f32)


def nt(a, b):
    return lax.dot_general(a, b, (((1,), (1,)), ((), ())), preferred_element_type=f32)


def pieces(values):
    high = values.astype(bf16).astype(f32)
    rest = values - high
    middle = rest.astype(bf16).astype(f32)
    low = (rest - middle).astype(bf16).astype(f32)
    return high, middle, low


def stack_left(ref, values):
    a, b, c = pieces(values)
    ref[...] = jnp.zeros_like(ref)
    for i, part in enumerate((a, a, b, a, c, b)):
        ref[8 * i : 8 * i + values.shape[0], :] = part


def stack_right(ref, values):
    a, b, c = pieces(values)
    ref[...] = jnp.zeros_like(ref)
    for i, part in enumerate((a, b, a, c, a, b)):
        ref[8 * i : 8 * i + values.shape[0], :] = part


def encoder_kernel(n, members, folded, block, *refs):
    step_ref, count_ref = refs[:2]
    sources, shards, out_ref = refs[2:15], refs[15:21], refs[21]
    locals_, refs = refs[22:35], refs[35:]
    slot_ref, recv_ref, rows_ref, geom_ref, mesh_ref = locals_[:5]
    cond_ref, target_ref, noise_ref, embed_ref, mesh_w_ref, geom_w_ref, noise_w_ref, film_w_ref = locals_[5:]
    w_ref, raw_ref, pick_ref, outgoing, arrived, embed_pad_ref, turn_ref = refs[:7]
    mesh_s_ref, mesh_k_ref, geom_s_ref, geom_k_ref, nodes_ref, ohr_ref, ohs_ref = refs[7:14]
    place_ref, meshg_ref, edges_ref, pre_ref, table_ref, mixed_ref, total_ref = refs[14:21]
    film_ref, received_ref = refs[21:23]
    z_recv, y_recv, x_recv, f_recv, c_recv, a_recv, sent_sem, in_sem, own_sem, heard = refs[23:]
    me = lax.axis_index("node")
    member = lax.axis_index("member")
    wide = 2 if folded else 1
    deep = n // 2 // wide
    core, chip = me % 2, me // 2
    y, z = chip % wide, chip // wide
    paired = members % 2 == 0
    x = member % 2 if paired else 0
    other_member = member + 1 - 2 * x
    width = w_ref.shape[3]
    part = width // 2 if paired else width

    def node_at(zz, yy, cc):
        return (zz * wide + yy) * 2 + cc

    def remote(source, target, way, recv, device):
        copy = pltpu.make_async_remote_copy(
            src_ref=source, dst_ref=target, send_sem=sent_sem.at[way], recv_sem=recv, device_id=device
        )
        copy.start()

    def arrive(like, sem):
        pltpu.make_async_copy(like, like, sem).wait()

    barrier = pltpu.get_barrier_semaphore()
    greeted = [{"node": node_at((z + j) % deep, y, core)} for j in range(1, deep)]
    greeted.append({"node": me + 1 - 2 * core})
    if wide == 2:
        greeted.append({"node": node_at(z, 1 - y, core)})
    if paired:
        greeted.append({"member": other_member})
    for device in greeted:
        pl.semaphore_signal(barrier, inc=1, device_id=device)
    loads = []
    for i, (source, target) in enumerate(zip(sources, locals_)):
        loads.append(pltpu.make_async_copy(source, target, in_sem.at[i]))

    def load(*which):
        for i in which:
            loads[i].start()

    def ready(*which):
        for i in which:
            loads[i].wait()

    load(2, 5, 6, 7)
    offsets = [0]
    mine = y * 2 + core
    for shard in shards:
        rows = shard.shape[0]
        target = w_ref.at[z, mine, pl.ds(offsets[-1], rows), :]
        pltpu.make_async_copy(shard, target, own_sem).start()
        offsets.append(offsets[-1] + rows)
    load(0, 1, 3, 4, 9, 10, 8, 11, 12)

    groups = [(offsets[k], offsets[k + 1]) for k in range(6)]
    near = x * part
    away = (1 - x) * part if paired else 0
    whole = ()
    every, others = pl.ds(0, deep), pl.ds(0, deep - 1)
    facing = (1 - y) * 2 + core
    partner = {"node": me + 1 - 2 * core}

    def halved(g):
        return paired and g not in whole

    def region(zz, lane, g, side):
        start, stop = groups[g]
        if not halved(g):
            return w_ref.at[zz, lane, pl.ds(start, stop - start), :]
        columns = pl.ds(pl.multiple_of(side, 128), part)
        return w_ref.at[zz, lane, pl.ds(start, stop - start), columns]

    def pass_core(g, lane, side):
        spot = region(every, lane, g, side)
        remote(spot, spot, 4, c_recv.at[g], partner)

    def start_z(g):
        for j in range(1, deep):
            spot = region(z, mine, g, near)
            remote(spot, spot, 0, z_recv.at[g], {"node": node_at((z + j) % deep, y, core)})

    def step_y(g):
        arrive(region(others, mine, g, near), z_recv.at[g])
        if wide == 2:
            spot = region(every, mine, g, near)
            remote(spot, spot, 1, y_recv.at[g], {"node": node_at(z, 1 - y, core)})
        if halved(g):
            for j in range(1, deep):
                spot = region((z + j) % deep, mine, g, near)
                remote(spot, spot, 2, x_recv.at[g], {"member": other_member})
        pass_core(g, mine, near)

    def step_x(g):
        if wide == 2:
            spot = region(every, facing, g, near)
            arrive(spot, y_recv.at[g])
            if halved(g):
                remote(spot, spot, 3, f_recv.at[g], {"member": other_member})
            pass_core(g, facing, near)

    def step_c(g):
        if halved(g):
            arrive(region(others, mine, g, away), x_recv.at[g])
            pass_core(g, mine, away)
            if wide == 2:
                arrive(region(every, facing, g, away), f_recv.at[g])
                pass_core(g, facing, away)

    def step_in(g):
        start, stop = groups[g]
        arrive(w_ref.at[:, pl.ds(0, wide), pl.ds(start, stop - start), :], c_recv.at[g])

    def weight(k):
        return w_ref[:, :, offsets[k] : offsets[k + 1], :].reshape(-1, width)

    channels = embed_ref.shape[0]
    cap = rows_ref.shape[1]
    listed = n * cap
    points, fixed = cond_ref.shape[1], cond_ref.shape[0]
    frac = jnp.full((1, 1), step_ref[0], jnp.int32).astype(f32) / (STEPS - 1)
    upper = sigma_top ** (1.0 / rho_power)
    lower = sigma_low ** (1.0 / rho_power)
    root = upper + frac * (lower - upper)
    cube = root * root * root
    sigma = cube * cube * root
    def make_picks():
        turn_ref[...] = jnp.zeros_like(turn_ref)
        raw_ref[...] = jnp.zeros_like(raw_ref)
        ready(2)
        turn_ref[:n, :cap] = rows_ref[...].astype(f32)
        turned = turn_ref[...].T
        spots = lax.broadcasted_iota(jnp.int32, (cap, points), 1).astype(f32)
        for r in range(n):
            chosen = turned[:cap, r : r + 1] == spots
            pick_ref[r * cap : (r + 1) * cap, :] = chosen.astype(f32).astype(bf16)
        ready(5, 6, 7)
        raw_ref[:fixed, :] = cond_ref[...].astype(f32)
        raw_ref[fixed:channels, :] = (target_ref[...] + sigma * noise_ref[...]) / jnp.sqrt(sigma * sigma + 1.0)
        outgoing[...] = nt(pick_ref[...], raw_ref[...].astype(bf16)).astype(bf16).reshape(outgoing.shape)

    def make_nodes():
        ready(4, 9)
        stack_left(mesh_s_ref, mesh_ref[...])
        stack_right(mesh_k_ref, mesh_w_ref[...])
        nodes_ref[...] = silu(nn(mesh_s_ref[...].T.astype(bf16), mesh_k_ref[...].astype(bf16))).astype(bf16)
        ready(3, 10)
        stack_left(geom_s_ref, geom_ref[...])
        stack_right(geom_k_ref, geom_w_ref[...])
        ready(0, 1)

    count = count_ref[0]
    nodes = mesh_ref.shape[1]
    blocks = geom_ref.shape[1] // block
    chunks = block // 128
    lanes = lax.broadcasted_iota(jnp.int32, (128, 128), 1).astype(f32)
    lane_row = lax.broadcasted_iota(jnp.int32, (1, 128), 1)
    node_rows = lax.broadcasted_iota(jnp.int32, (nodes, 128), 0).astype(f32)

    def prepare(b, carry):
        for c in range(chunks):
            j = b * chunks + c
            here = pl.ds(c * 128, 128)
            from_row = slot_ref[pl.ds(j, 1), :].astype(f32)
            to_row = jnp.where(j * 128 + lane_row < count, recv_ref[pl.ds(j, 1), :], -1).astype(f32)
            from_cols = jnp.broadcast_to(from_row, (128, 128)).T
            to_cols = jnp.broadcast_to(to_row, (128, 128)).T
            for t in range(listed // 128):
                ohs_ref[b, here, t * 128 : (t + 1) * 128] = (from_cols == lanes + 128.0 * t).astype(f32).astype(bf16)
            for t in range(nodes // 128):
                ohr_ref[here, t * 128 : (t + 1) * 128] = (to_cols == lanes + 128.0 * t).astype(f32).astype(bf16)
            place_ref[b, :, here] = (node_rows == to_row).astype(f32).astype(bf16)
        meshg_ref[b] = nn(ohr_ref[...], nodes_ref[...]).astype(bf16)
        here = pl.ds(pl.multiple_of(b * block, block), block)
        embedded = nn(geom_s_ref[:, here].T.astype(bf16), geom_k_ref[...].astype(bf16))
        edges_ref[b] = silu(embedded).astype(bf16)
        return carry

    def prepare_to(start, stop):
        lax.fori_loop(blocks * start // 8, blocks * stop // 8, prepare, 0)

    def start_exchange():
        for step in range(1, n):
            other = (me + step) % n
            remote(outgoing.at[other], arrived.at[me], 5, a_recv, {"node": other})

    stay = pltpu.make_async_copy(outgoing.at[me], arrived.at[me], in_sem.at[2])

    def start_local(_, carry):
        make_picks()
        make_nodes()
        return carry

    def end_exchange():
        stay.wait()
        arrive(arrived.at[pl.ds(0, n - 1)], a_recv)

    def prepare_noise():
        ready(11, 12)
        freqs = noise_w_ref.shape[0] // 2
        place_k = lax.broadcasted_iota(jnp.int32, (2 * freqs, 1), 0)
        wave = (place_k % freqs + 1).astype(f32)
        angle = 0.25 * jnp.log(sigma) * wave
        fourier = jnp.where(place_k < freqs, jnp.sin(angle), jnp.cos(angle))
        cond = silu(jnp.sum(fourier * noise_w_ref[...], axis=0, keepdims=True)).astype(bf16)
        film = nn(cond, film_w_ref[...])
        film_ref[...] = film
        ready(8)
        embed_pad_ref[...] = jnp.zeros_like(embed_pad_ref)
        embed_pad_ref[:channels, :] = embed_ref[...]

    def receive():
        end_exchange()
        listing = arrived[...].reshape(listed, arrived.shape[2])
        received_ref[...] = silu(nn(listing, embed_pad_ref[...])).astype(bf16)

    def rows_of(b):
        return pl.ds(pl.multiple_of(b * block, block), block)

    def edge_part(b, carry):
        pre_ref[rows_of(b), :] = nn(edges_ref[b], weight(0))
        return carry

    def node_part(b, carry):
        pre_ref[rows_of(b), :] += nn(meshg_ref[b], weight(1))
        return carry

    def make_table():
        table_ref[...] = nn(received_ref[...], weight(2)).astype(bf16)

    def hidden_part(b, carry):
        pre = pre_ref[rows_of(b), :] + nn(ohs_ref[b], table_ref[...])
        edges_ref[b] = silu(pre).astype(bf16)
        return carry

    def film_row(k):
        return film_ref[:, width * k : width * (k + 1)]

    def mix(b):
        mixed_ref[b % 2] = nn(edges_ref[b], weight(3))

    def message_part(b):
        if b + 1 < blocks:
            mix(b + 1)
        message = normalised(mixed_ref[b % 2]) * (1.0 + film_row(0)) + film_row(1)
        total_ref[...] += nn(place_ref[b], message.astype(bf16))

    def loop(body, start, stop, unroll=2):
        first, last = blocks * start // 8, blocks * stop // 8
        unroll = min(unroll, last - first)
        if (last - first) % unroll:
            unroll = 1

        def several(i, carry):
            for u in range(unroll):
                body(first + unroll * i + u, carry)
            return carry

        lax.fori_loop(0, (last - first) // unroll, several, 0)

    arrive(w_ref.at[z, mine], own_sem)
    pl.semaphore_wait(barrier, len(greeted))
    pl.semaphore_signal(heard.at[0], inc=1, device_id=partner)
    start_z(0)
    start_z(1)
    start_z(2)
    start_z(3)
    pl.semaphore_wait(heard.at[0], 1)
    if wide == 2:
        pl.semaphore_signal(heard.at[1], inc=1, device_id={"node": node_at(z, 1 - y, core)})
    make_picks()
    if wide == 2:
        pl.semaphore_wait(heard.at[1], 1)
    start_exchange()
    stay.start()
    start_z(5)
    start_z(4)
    make_nodes()
    step_y(0)
    loop(prepare, 0, 1, 1)
    step_y(1)
    loop(prepare, 1, 2, 1)
    step_x(0)
    step_y(2)
    loop(prepare, 2, 3, 1)
    step_x(1)
    prepare_noise()
    step_y(3)
    loop(prepare, 3, 4, 1)
    step_x(2)
    loop(prepare, 4, 5, 1)
    step_c(0)
    step_x(3)
    loop(prepare, 5, 6, 1)
    step_c(1)
    loop(prepare, 6, 7, 1)
    receive()
    step_y(5)
    loop(prepare, 7, 8, 1)
    step_in(0)
    loop(edge_part, 0, 4, 8)
    step_c(2)
    step_y(4)
    loop(edge_part, 4, 8, 8)
    step_x(5)
    step_in(1)
    step_c(3)
    loop(node_part, 0, 8, 8)
    step_x(4)
    step_in(2)
    make_table()
    loop(hidden_part, 0, 8, 8)
    step_in(3)
    total_ref[...] = jnp.zeros_like(total_ref)
    mix(0)
    for b in range(blocks * 0 // 8, blocks * 2 // 8):
        message_part(b)
    step_c(5)
    for b in range(blocks * 2 // 8, blocks * 4 // 8):
        message_part(b)
    step_c(4)
    for b in range(blocks * 4 // 8, blocks * 8 // 8):
        message_part(b)
    step_in(5)
    step_in(4)
    joint = weight(5)
    update = nn(nodes_ref[...], joint[:width]) + nn(total_ref[...].astype(bf16), joint[width:])
    update = silu(update).astype(bf16)
    result = normalised(nn(update, weight(4))) * (1.0 + film_row(2)) + film_row(3)
    out_ref[...] = (nodes_ref[...].astype(f32) + result).astype(bf16)
    for g in range(6):
        arrive(region(others, mine, g, near), sent_sem.at[0])
        if wide == 2:
            arrive(region(every, mine, g, near), sent_sem.at[1])
        if halved(g):
            arrive(region(others, mine, g, near), sent_sem.at[2])
            if wide == 2:
                arrive(region(every, mine, g, near), sent_sem.at[3])
    arrive(w_ref.at[:, pl.ds(0, wide), :, :], sent_sem.at[4])
    arrive(arrived.at[pl.ds(0, n - 1)], sent_sem.at[5])


def per_device(n, members, folded, *args):
    conditioning, target_state, noise_sample, step_index, mesh_features, edge_geometry = args[:6]
    edge_slot, edge_receiver, send_rows, edge_count, embed_weight, mesh_weight, geom_weight = args[6:13]
    sender_w, edge_w, receiver_w, message_w, node_w, output_w = args[13:19]
    noise_weight, film_weight = args[19:]
    shards = (edge_w, receiver_w, sender_w, message_w, output_w, node_w)
    channels, width = embed_weight.shape
    nodes, edges = mesh_features.shape[1], edge_geometry.shape[1]
    cap = send_rows.shape[1]
    points = conditioning.shape[1]
    listed = n * cap
    deep = channels + -channels % 128
    block = min(512, edges)
    blocks = edges // block
    lines = 2 if folded else 1
    layers = n // 2 // lines
    stacked = sum(shard.shape[0] for shard in shards)
    inputs = (
        edge_slot.reshape(-1, 128),
        edge_receiver.reshape(-1, 128),
        send_rows,
        edge_geometry,
        mesh_features,
        conditioning,
        target_state,
        noise_sample,
        embed_weight,
        mesh_weight,
        geom_weight,
        noise_weight,
        film_weight,
    )
    dma = pltpu.SemaphoreType.DMA
    vmem = pl.BlockSpec(memory_space=pltpu.VMEM)
    smem = pl.BlockSpec(memory_space=pltpu.SMEM)
    hbm = pl.BlockSpec(memory_space=pltpu.HBM)
    return pl.pallas_call(
        functools.partial(encoder_kernel, n, members, folded, block),
        out_shape=jax.ShapeDtypeStruct((nodes, width), bf16),
        in_specs=[smem] * 2 + [hbm] * 19,
        out_specs=vmem,
        scratch_shapes=[pltpu.VMEM(value.shape, value.dtype) for value in inputs]
        + [
            pltpu.VMEM((layers, 2 * lines, stacked, width), bf16),
            pltpu.VMEM((deep, points), f32),
            pltpu.VMEM((listed, points), bf16),
            pltpu.VMEM((n, cap, deep), bf16),
            pltpu.VMEM((n, cap, deep), bf16),
            pltpu.VMEM((deep, width), bf16),
            pltpu.VMEM((128, 128), f32),
            pltpu.VMEM((128, nodes), f32),
            pltpu.VMEM((128, width), f32),
            pltpu.VMEM((128, edges), f32),
            pltpu.VMEM((128, width), f32),
            pltpu.VMEM((nodes, width), bf16),
            pltpu.VMEM((block, nodes), bf16),
            pltpu.VMEM((blocks, block, listed), bf16),
            pltpu.VMEM((blocks, nodes, block), bf16),
            pltpu.VMEM((blocks, block, width), bf16),
            pltpu.VMEM((blocks, block, width), bf16),
            pltpu.VMEM((edges, width), f32),
            pltpu.VMEM((listed, width), bf16),
            pltpu.VMEM((2, block, width), f32),
            pltpu.VMEM((nodes, width), f32),
            pltpu.VMEM((1, 4 * width), f32),
            pltpu.VMEM((listed, width), bf16),
            dma((6,)),
            dma((6,)),
            dma((6,)),
            dma((6,)),
            dma((6,)),
            dma,
            dma((6,)),
            dma((13,)),
            dma,
            pltpu.SemaphoreType.REGULAR((2,)),
        ],
        compiler_params=pltpu.CompilerParams(collective_id=0, has_side_effects=True),
    )(step_index, edge_count, *inputs, *shards)


def solution(mesh):
    placed = (
        P(None, ("member", "node")),
        P(None, ("member", "node")),
        P(None, ("member", "node")),
        P("member"),
        P(None, "node"),
        P(None, "node"),
        P("node"),
        P("node"),
        P("node", None),
        P("node"),
        P(),
        P(),
        P(),
        P("node", None),
        P("node", None),
        P("node", None),
        P("node", None),
        P("node", None),
        P("node", None),
        P(),
        P(),
    )
    body = functools.partial(per_device, mesh.shape["node"], mesh.shape["member"], is_folded(mesh))
    return jax.shard_map(
        body, mesh=mesh, in_specs=placed, out_specs=P("node", "member"), check_vma=False
    )
```
